512 devices in a mesh: parts: 2 (over y), seq: 32 (over z), tp: 8 (over x, core).
Axes of the slice: x: 4, y: 2, z: 32, core: 2. Of those that a mesh axis runs over, the one named last changes fastest.
The devices are a block of a 4x8x32 slice.
Arguments:
- tokens: bfloat16 [16384, 8192], P(('parts', 'seq'), 'tp'), parts along dimension 0, may hold values from -6 to 6
- norm_gain: bfloat16 [8192], P('tp'), may hold values from 0.099609375 to 1.8984375
- w_query: bfloat16 [8192, 4096], P('seq', 'tp'), may hold values from -0.0625 to 0.0625
- w_kv: bfloat16 [8192, 2, 1024], P('seq', None, 'tp'), may hold values from -0.0625 to 0.0625
- b_query: float32 [4096], P('tp'), may hold values from -4 to 4
- b_kv: float32 [2, 1024], P(None, 'tp'), may hold values from -4 to 4
- kv_pool: bfloat16 [8192, 2, 8, 1024], P(('parts', 'seq'), None, None, 'tp'), parts along dimension 0, may hold values from -68 to 68
- prefix_pages: int32 [128, 32], P('parts'), parts along dimension 0, may hold values from 0 to 4095, as said below
- prefix_len: int32 [128], P('parts'), parts along dimension 0, may hold values from 0 to 256
- suffix_len: int32 [128], P('parts'), parts along dimension 0, may hold values from 1 to 128
- fresh_owner: int32 [2048, 1], P('parts'), parts along dimension 0, may hold values from 0 to 31; in each aligned block of 32 rows (0 to 31, 32 to 63, ...) at most 2 rows name the same one
Outputs:
- attn_out: bfloat16 [16384, 4096], P(('parts', 'seq'), 'tp'), parts along dimension 0
- fresh_pages: bfloat16 [4096, 2, 8, 1024], P(('parts', 'seq'), None, None, 'tp'), parts along dimension 0
The draws below stay inside these ranges and needn't reach their ends.
There are 2 independent parts, one for each index of `parts`. The reference program is written for one: setup_inputs(seed, part) draws one part's arguments, and reference() takes and returns one part's arrays. A program takes and returns all parts, laid end to end along the dimension named above; an argument that names none is the same for every part. Nothing has to cross between parts.
Inputs may be any that keep to these rules, and one draw needn't show every extreme that they name: `prefix_pages`: page id q lies in the 128 pages of sequence group q // 128. Among the 64 entries of requests 2*g to 2*(g+1)-1, no group holds more than 3, and in every such block some group holds exactly 3. Entries past the matched prefix still name pages. `fresh_owner`: in the rows of one sequence group's requests (aligned blocks of 32 rows) no group is named more than 2 times; some blocks name one exactly 2 times.
All inputs are finite; a program needn't handle non-finite values.
Results may differ from the reference program's by a relative error of at most 0.005.
The reference program's roundings to bfloat16 on the way (of `normed` and `probs`) count: a program that leaves them out, or rounds other values in their place, can miss the bound.
Values may be sent and summed in bfloat16 or wider, within the bound.
No kernel may reach another device: no remote copies, remote signals or barrier semaphores. Data moves between devices by JAX's collectives and lax.ppermute only.
A program may use at most 64 MiB of HBM per device.

```python
import math
import jax
import jax.numpy as jnp
import numpy as np
from jax import lax

D = 8192
HEADS = 32
KV_HEADS = 8
HEAD_DIM = 128
BLOCK = 128
PAGE = 8
PMAX = 32
BLK_DEV = 2
PAGES_DEV = 128
REQS = 64
TOKENS = 8192
SUF_PAGES = 16
POOL = 4096
C_PRE = 3
C_NEW = 2
FRESH = 2048
N_SEQ = 32


def draw_prefix_pages(key, part):
    entries = BLK_DEV * PMAX
    items = C_PRE * N_SEQ

    def one_block(block_key):
        first_key, second_key, third_key, fourth_key = jax.random.split(block_key, 4)
        order = jax.random.permutation(first_key, N_SEQ).astype(jnp.int32)
        item_ids = jnp.arange(items, dtype=jnp.int32)
        owner_of = order[item_ids % N_SEQ]
        scores = jax.random.randint(second_key, (items,), 1, 1 << 20, dtype=jnp.int32)
        scores = jnp.where(item_ids % N_SEQ == 0, 0, scores)
        picked = jnp.argsort(scores * items + item_ids, stable=True)[:entries]
        owners = owner_of[picked]
        owners = owners[jax.random.permutation(third_key, entries)]
        slots = jax.random.randint(fourth_key, (entries,), 0, PAGES_DEV, dtype=jnp.int32)
        return (owners * PAGES_DEV + slots).astype(jnp.int32)
    block_keys = jax.random.split(jax.random.fold_in(key, 11), N_SEQ)
    return jax.vmap(one_block)(block_keys).reshape(REQS, PMAX)


def draw_kv_pool(key, part):
    shape = (POOL, 2, PAGE, KV_HEADS * HEAD_DIM)
    first_key = jax.random.fold_in(jax.random.fold_in(key, 23), 0)
    return jnp.clip(jax.random.normal(first_key, shape, jnp.float32), -6.0, 6.0).astype(jnp.bfloat16)


def set_ends(values, rng, low, high):
    place = [jax.random.randint(jax.random.fold_in(rng, axis), (), 0, length) for axis, length in enumerate(values.shape)]
    widest = values.shape.index(max(values.shape))
    beside = place[:widest] + [(place[widest] + 1) % values.shape[widest]] + place[widest + 1:]
    return values.at[tuple(place)].set(low).at[tuple(beside)].set(high)


def shard_levels(rng, shape, cuts, smallest, top_value):
    loudness = 1.0
    for dim, blocks in cuts:
        steps = jax.random.uniform(jax.random.fold_in(jax.random.fold_in(rng, 6), dim), (blocks,), jnp.float32, smallest / len(cuts), top_value / len(cuts))
        loudness = loudness * jnp.repeat(jnp.exp(steps), shape[dim] // blocks).reshape((-1,) + (1,) * (len(shape) - 1 - dim))
    return loudness


def deal_out(stream_key, own, number, rows, count, top, bound, lean):
    order = jax.random.permutation(stream_key, count)
    crowded, usual = load_shares(count, rows * top, bound, lean, True), load_shares(count, rows * top, bound, lean, False)
    places = jnp.arange(count)

    def named(tallies, turn):
        used = int((tallies > 0).sum())
        fixed = max(1, used // 4)
        passed = fixed + (places - fixed + turn * (used - fixed)) % max(1, count - fixed)
        return jnp.zeros((count,), jnp.int32).at[order[jnp.where(places < fixed, places, passed)]].set(jnp.asarray(tallies, jnp.int32))

    tallies = jnp.where(number % 4 == 0, named(crowded, number // 4), named(usual, number - number // 4 - 1))
    mixed = jax.random.permutation(jax.random.fold_in(own, 3), count)
    giver, receiver = mixed[0:count // 2 * 2:2], mixed[1:count // 2 * 2:2]
    slack = jnp.minimum(tallies[giver] - 1, bound - tallies[receiver]) // 2
    slack = jnp.where((giver == order[0]) | (receiver == order[0]) | (tallies[receiver] == 0), 0, jnp.maximum(slack, 0))
    passed = jax.random.randint(jax.random.fold_in(own, 4), (count // 2,), 0, 1 << 20) % (slack + 1)
    tallies = tallies.at[giver].add(-passed).at[receiver].add(passed)
    labels = jnp.searchsorted(jnp.cumsum(tallies), jnp.arange(rows * top), side="right").astype(jnp.int32)
    grid = labels.reshape(top, rows).T
    grid = grid[jax.random.permutation(jax.random.fold_in(own, 1), rows)]
    turn = jax.random.randint(jax.random.fold_in(own, 2), (rows, 1), 0, top)
    return jnp.take_along_axis(grid, (jnp.arange(top)[None, :] + turn) % top, axis=1)


def load_shares(amount, total, bound, slope, full):
    portions = [(1 << 20) // math.isqrt(standing ** slope) + 1 for standing in range(1, amount + 1)]
    largest = bound if full else min(bound, max(-(-total // amount), total * portions[0] // sum(portions)))
    least = 1 if total - largest >= amount - 1 else 0
    holding, spare = [largest] + [least] * (amount - 1), total - largest - least * (amount - 1)
    while spare > 0:
        free = [i for i in range(1, amount) if holding[i] < largest] or [i for i in range(1, amount) if holding[i] < bound]
        whole, left = sum([portions[i] for i in free]), spare
        for i in free:
            more = min(bound - holding[i], max(1, left * portions[i] // whole), spare)
            holding[i] = holding[i] + more
            spare = spare - more
    return np.array(holding)


def normal_values(stream_key, dims, deviation, reach, pieces=(), kind=jnp.bfloat16):
    loudness = shard_levels(stream_key, dims, pieces, -0.22, 0.18) if pieces else 1.0
    result = jax.random.normal(stream_key, dims, jnp.float32) * deviation * loudness
    return jnp.minimum(jnp.maximum(result, -reach), reach).astype(kind)


def setup_inputs(seed: int = 0, part: int = 0) -> dict:
    key_list = jax.random.split(jax.random.key(seed), 12)
    own_keys = jax.random.split(jax.random.fold_in(key_list[11], part), 12)
    tokens = normal_values(own_keys[0], (TOKENS, D), 1.0, 6.0, ((0, 32), (1, 8)))
    norm_gain = jnp.clip(1.0 + 0.18 * jax.random.normal(key_list[1], (D,), jnp.float32), 0.099609375, 1.8984375).astype(jnp.bfloat16)
    w_query = normal_values(key_list[2], (D, HEADS * HEAD_DIM), D ** -0.5, 0.0625, ((0, 32), (1, 8)))
    w_kv = normal_values(key_list[3], (D, 2, KV_HEADS * HEAD_DIM), D ** -0.5, 0.0625, ((0, 32), (2, 8)))
    b_query = normal_values(key_list[4], (HEADS * HEAD_DIM,), 1.0, 4.0, ((0, 8),), jnp.float32)
    b_kv = normal_values(key_list[5], (2, KV_HEADS * HEAD_DIM), 1.0, 4.0, ((1, 8),), jnp.float32)
    kv_pool = draw_kv_pool(jax.random.fold_in(jax.random.fold_in(key_list[11], part), 71), part)
    prefix_pages = draw_prefix_pages(jax.random.fold_in(jax.random.fold_in(key_list[11], part), 71), part)
    prefix_len = set_ends(jax.random.randint(own_keys[8], (REQS,), 0, PMAX * PAGE + 1), jax.random.fold_in(own_keys[8], 1), 0, PMAX * PAGE).astype(jnp.int32)
    suffix_len = set_ends(jax.random.randint(own_keys[9], (REQS,), 1, BLOCK + 1), jax.random.fold_in(own_keys[9], 1), 1, BLOCK).astype(jnp.int32)
    fresh_owner_keys = jax.random.split(jax.random.fold_in(own_keys[10], 1), (REQS * SUF_PAGES) // (BLK_DEV * SUF_PAGES))
    fresh_owner_turns = jax.random.permutation(jax.random.fold_in(own_keys[10], 3), (REQS * SUF_PAGES) // (BLK_DEV * SUF_PAGES))
    fresh_owner = jax.vmap(lambda own, number: deal_out(jax.random.fold_in(own_keys[10], 2), own, number, BLK_DEV * SUF_PAGES, N_SEQ, 1, C_NEW, 2))(fresh_owner_keys, fresh_owner_turns).reshape((REQS * SUF_PAGES, 1))
    return {"tokens": tokens, "norm_gain": norm_gain, "w_query": w_query, "w_kv": w_kv, "b_query": b_query, "b_kv": b_kv, "kv_pool": kv_pool, "prefix_pages": prefix_pages, "prefix_len": prefix_len, "suffix_len": suffix_len, "fresh_owner": fresh_owner}


def rotate(values, positions):
    half_dim = values.shape[-1] // 2
    freq_index = jnp.arange(half_dim, dtype=jnp.float32)
    inverse = jnp.exp(freq_index * (-2.0 * math.log(1000000.0) / values.shape[-1]))
    angles = positions.astype(jnp.float32)[..., None, None] * inverse
    cosine = jnp.cos(angles)
    sine = jnp.sin(angles)
    first_half = values[..., :half_dim]
    second_half = values[..., half_dim:]
    return jnp.concatenate([first_half * cosine - second_half * sine, second_half * cosine + first_half * sine], axis=-1)

def attend(query, key_new, value_new, key_old, value_old, prefix_mine, suffix_mine):
    batch, block_len, heads_here, head_dim = query.shape
    kv_here = key_new.shape[2]
    group_size = heads_here // kv_here
    old_len = key_old.shape[1]
    grouped = query.reshape(batch, block_len, kv_here, group_size, head_dim)
    all_keys = jnp.concatenate([key_old, key_new], axis=1)
    all_values = jnp.concatenate([value_old, value_new], axis=1)
    scores = jnp.einsum('btkgd,bskd->bkgts', grouped.astype(jnp.float32), all_keys.astype(jnp.float32)) / math.sqrt(head_dim)
    key_pos = jnp.arange(old_len + block_len, dtype=jnp.int32)
    query_pos = jnp.arange(block_len, dtype=jnp.int32)
    in_prefix = key_pos[None, None, :] < prefix_mine[:, None, None]
    shifted = key_pos - old_len
    in_suffix = (shifted[None, None, :] <= query_pos[None, :, None]) & (shifted[None, None, :] < suffix_mine[:, None, None])
    allowed = jnp.where(key_pos[None, None, :] < old_len, in_prefix, in_suffix)[:, None, None]
    masked = jnp.where(allowed, scores, -1e+30)
    peak = lax.optimization_barrier(jnp.max(masked, axis=-1, keepdims=True))
    weights = jnp.where(allowed, jnp.exp(masked - peak), 0.0)
    probs = (weights / lax.optimization_barrier(jnp.sum(weights, axis=-1, keepdims=True))).astype(jnp.bfloat16)
    mixed = jnp.einsum('bkgts,bskd->btkgd', probs.astype(jnp.float32), all_values.astype(jnp.float32))
    live = query_pos[None, :] < suffix_mine[:, None]
    mixed = jnp.where(live[:, :, None, None, None], mixed, 0.0)
    return mixed.reshape(batch * block_len, heads_here * head_dim).astype(jnp.bfloat16)

def reference(tokens, norm_gain, w_query, w_kv, b_query, b_kv, kv_pool, prefix_pages, prefix_len, suffix_len, fresh_owner):
    kv_width = KV_HEADS * HEAD_DIM
    widened = tokens.astype(jnp.float32)
    mean_square = lax.optimization_barrier(jnp.mean(widened * widened, axis=-1, keepdims=True))
    normed = (widened * lax.rsqrt(mean_square + 1e-06) * norm_gain.astype(jnp.float32)).astype(jnp.bfloat16)
    query_lin = jnp.dot(normed, w_query, preferred_element_type=jnp.float32) + b_query
    pair_lin = jnp.dot(normed, w_kv.reshape(D, 2 * kv_width), preferred_element_type=jnp.float32) + b_kv.reshape(2 * kv_width)
    slot_ids = jnp.arange(BLOCK, dtype=jnp.int32)
    positions = prefix_len[:, None] + slot_ids[None, :]
    live = (slot_ids[None, :] < suffix_len[:, None])[:, :, None, None]
    query = rotate(query_lin.reshape(REQS, BLOCK, HEADS, HEAD_DIM), positions).astype(jnp.bfloat16)
    key_new = jnp.where(live, rotate(pair_lin[:, :kv_width].reshape(REQS, BLOCK, KV_HEADS, HEAD_DIM), positions), 0.0).astype(jnp.bfloat16)
    value_new = jnp.where(live, pair_lin[:, kv_width:].reshape(REQS, BLOCK, KV_HEADS, HEAD_DIM), 0.0).astype(jnp.bfloat16)

    def one_request(packed):
        query_one, key_one, value_one, page_row, prefix_one, suffix_one = packed
        pages = kv_pool[page_row]
        key_old = pages[:, 0].reshape(1, PMAX * PAGE, KV_HEADS, HEAD_DIM)
        value_old = pages[:, 1].reshape(1, PMAX * PAGE, KV_HEADS, HEAD_DIM)
        return attend(query_one[None], key_one[None], value_one[None], key_old, value_old, prefix_one[None], suffix_one[None])
    attn_out = lax.map(one_request, (query, key_new, value_new, prefix_pages, prefix_len, suffix_len))
    attn_out = attn_out.reshape(TOKENS, HEADS * HEAD_DIM)
    new_pages = jnp.stack([key_new.reshape(REQS * SUF_PAGES, PAGE, kv_width), value_new.reshape(REQS * SUF_PAGES, PAGE, kv_width)], axis=1)
    owners = fresh_owner[:, 0].reshape(N_SEQ, BLK_DEV * SUF_PAGES)
    order_ids = jnp.arange(BLK_DEV * SUF_PAGES, dtype=jnp.int32)
    earlier = (owners[:, :, None] == owners[:, None, :]) & (order_ids[None, None, :] < order_ids[None, :, None])
    ranks = lax.optimization_barrier(jnp.sum(earlier.astype(jnp.int32), axis=-1))
    groups = jnp.arange(N_SEQ, dtype=jnp.int32)[:, None]
    target = ((owners * N_SEQ + groups) * C_NEW + ranks).reshape(-1).astype(jnp.int32)
    fresh_pages = jnp.zeros((FRESH, 2, PAGE, kv_width), jnp.bfloat16).at[target].set(new_pages)
    return (attn_out, fresh_pages)
```

```python
import math

import jax
import jax.numpy as jnp
from jax import lax
from jax.sharding import PartitionSpec as P

HEAD_DIM = 128
BLOCK = 128
PAGE = 8
CORES = 2


def rotate(values, positions):
    half_dim = values.shape[-1] // 2
    freq_index = jnp.arange(half_dim, dtype=jnp.float32)
    inverse = jnp.exp(freq_index * (-2.0 * math.log(1000000.0) / values.shape[-1]))
    angles = positions.astype(jnp.float32)[..., None, None] * inverse
    cosine = jnp.cos(angles)
    sine = jnp.sin(angles)
    first_half = values[..., :half_dim]
    second_half = values[..., half_dim:]
    return jnp.concatenate(
        [first_half * cosine - second_half * sine, second_half * cosine + first_half * sine],
        axis=-1,
    )


def attend(query, key_new, value_new, key_old, value_old, prefix_mine, suffix_mine):
    batch, block_len, heads_here, head_dim = query.shape
    kv_here = key_new.shape[2]
    group_size = heads_here // kv_here
    old_len = key_old.shape[1]
    grouped = query.reshape(batch, block_len, kv_here, group_size, head_dim)
    all_keys = jnp.concatenate([key_old, key_new], axis=1)
    all_values = jnp.concatenate([value_old, value_new], axis=1)
    scores = jnp.einsum(
        "btkgd,bskd->bkgts", grouped, all_keys, preferred_element_type=jnp.float32
    ) / math.sqrt(head_dim)
    key_pos = jnp.arange(old_len + block_len, dtype=jnp.int32)
    query_pos = jnp.arange(block_len, dtype=jnp.int32)
    in_prefix = key_pos[None, None, :] < prefix_mine[:, None, None]
    shifted = key_pos - old_len
    in_suffix = (shifted[None, None, :] <= query_pos[None, :, None]) & (
        shifted[None, None, :] < suffix_mine[:, None, None]
    )
    allowed = jnp.where(key_pos[None, None, :] < old_len, in_prefix, in_suffix)[:, None, None]
    masked = jnp.where(allowed, scores, -1e30)
    peak = jnp.max(masked, axis=-1, keepdims=True)
    weights = jnp.where(allowed, jnp.exp(masked - peak), 0.0)
    probs = (weights / jnp.sum(weights, axis=-1, keepdims=True)).astype(jnp.bfloat16)
    mixed = jnp.einsum("bkgts,bskd->btkgd", probs, all_values, preferred_element_type=jnp.float32)
    live = query_pos[None, :] < suffix_mine[:, None]
    mixed = jnp.where(live[:, :, None, None, None], mixed, 0.0)
    return mixed.reshape(batch * block_len, heads_here * head_dim).astype(jnp.bfloat16)


def swap_parts(value):
    count = lax.axis_size("parts")
    return lax.ppermute(value, "parts", [(i, i ^ 1) for i in range(count)])


def swap_cores(value):
    count = lax.axis_size("tp")
    return lax.ppermute(value, "tp", [(i, i ^ 1) for i in range(count)])


def shift_chips(value, by):
    count = lax.axis_size("tp")
    return lax.ppermute(value, "tp", [(i, (i + by * CORES) % count) for i in range(count)])


def gather_chips(own):
    half = own.shape[0] // 2
    from_left = shift_chips(own, 1)
    from_right = shift_chips(own, -1)
    own_other = swap_cores(own)
    far_top = shift_chips(from_left[:half], 1)
    far_low = shift_chips(from_right[half:], -1)
    left_other = swap_cores(from_left)
    right_other = swap_cores(from_right)
    far = jnp.concatenate([far_top, far_low], axis=0)
    far_other = swap_cores(far)
    return [
        (own, own_other),
        (from_left, left_other),
        (from_right, right_other),
        (far, far_other),
    ]


STEPS = (0, -1, 1, 2)


def body(
    tokens,
    norm_gain,
    w_query,
    w_kv,
    b_query,
    b_kv,
    kv_pool,
    prefix_pages,
    prefix_len,
    suffix_len,
    fresh_owner,
):
    seq_count = lax.axis_size("seq")
    tp_count = lax.axis_size("tp")
    my_group = lax.axis_index("seq")
    my_tp = lax.axis_index("tp")
    parity = lax.axis_index("parts") % 2
    token_rows, feat = tokens.shape
    blocks_here = token_rows // BLOCK
    kv_width = w_kv.shape[2]
    kv_here = kv_width // HEAD_DIM
    query_width = w_query.shape[1]
    half_width = query_width // 2
    heads_here = query_width // HEAD_DIM
    half_heads = heads_here // 2
    pool_pages = kv_pool.shape[0]
    page_slots = prefix_pages.shape[1]
    prefix_entries = blocks_here * page_slots
    suffix_pages = BLOCK // PAGE
    fresh_entries = blocks_here * suffix_pages
    prefix_cap = max(3, prefix_entries // seq_count + 1)
    fresh_cap = max(2, (fresh_entries + seq_count - 1) // seq_count + 1)
    first_row = my_group * blocks_here
    prefix_mine = lax.dynamic_slice_in_dim(prefix_len, first_row, blocks_here)
    suffix_mine = lax.dynamic_slice_in_dim(suffix_len, first_row, blocks_here)
    owners_mine = lax.dynamic_slice_in_dim(
        fresh_owner[:, 0], first_row * suffix_pages, fresh_entries
    )

    w_pair_half = lax.dynamic_index_in_dim(w_kv, parity, 1, keepdims=False)
    w_query_half = lax.dynamic_slice_in_dim(w_query, parity * half_width, half_width, axis=1)
    w_pair_all = lax.all_gather(w_pair_half, "seq", axis=0, tiled=True)
    w_query_all = lax.all_gather(w_query_half, "seq", axis=0, tiled=True)
    b_pair_half = lax.dynamic_index_in_dim(b_kv, parity, 0, keepdims=True)
    b_query_half = lax.dynamic_slice_in_dim(b_query, parity * half_width, half_width)[None]

    gain_rows = jnp.broadcast_to(norm_gain[None], (16, feat))
    mine_ext = jnp.concatenate([gain_rows, tokens], axis=0)
    other_tokens = swap_parts(tokens)
    other_prefix = swap_parts(prefix_mine)
    pieces_mine = gather_chips(mine_ext)
    pieces_other = gather_chips(other_tokens)

    square = jnp.zeros((2 * token_rows, 1), jnp.float32)
    raw = []
    for mine, other, step in zip(pieces_mine, pieces_other, STEPS):
        for core in range(CORES):
            rows = jnp.concatenate([mine[core][16:], other[core]], axis=0)
            gain = mine[core][:1]
            at = ((my_tp + step * CORES) % tp_count) ^ core
            wide = rows.astype(jnp.float32)
            square = square + jnp.sum(wide * wide, axis=-1, keepdims=True)
            raw.append((rows, gain, at))
    scale = lax.rsqrt(square / (feat * tp_count) + 1e-06)
    normed = jnp.zeros((2 * token_rows, feat * tp_count), jnp.bfloat16)
    for rows, gain, at in raw:
        done = (rows.astype(jnp.float32) * scale * gain.astype(jnp.float32)).astype(jnp.bfloat16)
        normed = lax.dynamic_update_slice_in_dim(normed, done, at * feat, axis=1)

    all_ids = prefix_pages.reshape(seq_count, prefix_entries)
    all_owner = all_ids // pool_pages
    entry_ids = jnp.arange(prefix_entries, dtype=jnp.int32)
    before = (all_owner[:, :, None] == all_owner[:, None, :]) & (
        entry_ids[None, None, :] < entry_ids[None, :, None]
    )
    all_rank = jnp.sum(before.astype(jnp.int32), axis=-1)
    prefix_slots = jnp.arange(prefix_cap, dtype=jnp.int32)
    chosen = (all_owner[:, None, :] == my_group) & (
        all_rank[:, None, :] == prefix_slots[None, :, None]
    )
    picked = jnp.sum(jnp.where(chosen, entry_ids[None, None, :], 0), axis=-1)
    local_page = jnp.take_along_axis(all_ids, picked, axis=1) % pool_pages
    prefix_send = kv_pool[local_page]
    prefix_got = lax.all_to_all(prefix_send, "seq", split_axis=0, concat_axis=0, tiled=True)

    slot_ids = jnp.arange(BLOCK, dtype=jnp.int32)
    both_prefix = jnp.concatenate([prefix_mine, other_prefix])
    positions = both_prefix[:, None] + slot_ids[None, :]
    live = (slot_ids[None, :] < suffix_mine[:, None])[:, :, None, None]
    pair_lin = jnp.dot(normed, w_pair_all, preferred_element_type=jnp.float32) + b_pair_half
    pair_lin = pair_lin.reshape(2 * blocks_here, BLOCK, kv_here, HEAD_DIM)
    pair_half = jnp.where(parity == 0, rotate(pair_lin, positions), pair_lin).astype(jnp.bfloat16)
    pair_kept = pair_half[:blocks_here]
    pair_got = swap_parts(pair_half[blocks_here:])
    zero = jnp.zeros((), jnp.bfloat16)
    key_new = jnp.where(live, jnp.where(parity == 0, pair_kept, pair_got), zero)
    value_new = jnp.where(live, jnp.where(parity == 0, pair_got, pair_kept), zero)

    new_pages = jnp.stack(
        [
            key_new.reshape(fresh_entries, PAGE, kv_width),
            value_new.reshape(fresh_entries, PAGE, kv_width),
        ],
        axis=1,
    )
    fresh_ids = jnp.arange(fresh_entries, dtype=jnp.int32)
    fresh_before = (owners_mine[None, :] == owners_mine[:, None]) & (
        fresh_ids[None, :] < fresh_ids[:, None]
    )
    fresh_rank = jnp.sum(fresh_before.astype(jnp.int32), axis=1)
    group_ids = jnp.arange(seq_count, dtype=jnp.int32)
    fresh_slots = jnp.arange(fresh_cap, dtype=jnp.int32)
    placed = (owners_mine[None, None, :] == group_ids[:, None, None]) & (
        fresh_rank[None, None, :] == fresh_slots[None, :, None]
    )
    source = jnp.sum(jnp.where(placed, fresh_ids[None, None, :], 0), axis=-1)
    filled = jnp.any(placed, axis=-1)
    fresh_send = jnp.where(filled[:, :, None, None, None], new_pages[source], zero)
    fresh_got = lax.all_to_all(fresh_send, "seq", split_axis=0, concat_axis=0, tiled=True)

    query_lin = jnp.dot(normed, w_query_all, preferred_element_type=jnp.float32) + b_query_half
    query_half = rotate(
        query_lin.reshape(2 * blocks_here, BLOCK, half_heads, HEAD_DIM), positions
    ).astype(jnp.bfloat16)
    query_kept = query_half[:blocks_here]
    query_got = swap_parts(query_half[blocks_here:])
    query = jnp.concatenate(
        [
            jnp.where(parity == 0, query_kept, query_got),
            jnp.where(parity == 0, query_got, query_kept),
        ],
        axis=2,
    )

    my_rank = lax.dynamic_index_in_dim(all_rank, my_group, 0, keepdims=False)
    my_ids = lax.dynamic_index_in_dim(all_ids, my_group, 0, keepdims=False)
    arrived_at = my_ids // pool_pages * prefix_cap + my_rank
    fetched = prefix_got.reshape(seq_count * prefix_cap, 2, PAGE, kv_width)[arrived_at]
    fetched = fetched.reshape(blocks_here, page_slots, 2, PAGE, kv_here, HEAD_DIM)
    key_old = fetched[:, :, 0].reshape(blocks_here, page_slots * PAGE, kv_here, HEAD_DIM)
    value_old = fetched[:, :, 1].reshape(blocks_here, page_slots * PAGE, kv_here, HEAD_DIM)
    attn_out = attend(query, key_new, value_new, key_old, value_old, prefix_mine, suffix_mine)
    fresh_out = fresh_got.reshape(seq_count * fresh_cap, 2, PAGE, kv_width)
    return (attn_out, fresh_out)


def solution(mesh):
    placed = (
        P(("parts", "seq"), "tp"),
        P("tp"),
        P("seq", "tp"),
        P("seq", None, "tp"),
        P("tp"),
        P(None, "tp"),
        P(("parts", "seq"), None, None, "tp"),
        P("parts", None),
        P("parts"),
        P("parts"),
        P("parts", None),
    )
    return jax.shard_map(
        body,
        mesh=mesh,
        in_specs=placed,
        out_specs=(P(("parts", "seq"), "tp"), P(("parts", "seq"), None, None, "tp")),
        check_vma=False,
    )
```

```python
import math

import jax
import jax.numpy as jnp
from jax import lax
from jax.sharding import PartitionSpec as P

HEAD_DIM = 128
BLOCK = 128
PAGE = 8
CORES = 2


def rotate(values, positions):
    half_dim = values.shape[-1] // 2
    freq_index = jnp.arange(half_dim, dtype=jnp.float32)
    inverse = jnp.exp(freq_index * (-2.0 * math.log(1000000.0) / values.shape[-1]))
    angles = positions.astype(jnp.float32)[..., None, None] * inverse
    cosine = jnp.cos(angles)
    sine = jnp.sin(angles)
    first_half = values[..., :half_dim]
    second_half = values[..., half_dim:]
    return jnp.concatenate(
        [first_half * cosine - second_half * sine, second_half * cosine + first_half * sine],
        axis=-1,
    )


def attend(query, key_new, value_new, key_old, value_old, prefix_mine, suffix_mine):
    batch, block_len, heads_here, head_dim = query.shape
    kv_here = key_new.shape[2]
    group_size = heads_here // kv_here
    old_len = key_old.shape[1]
    grouped = query.reshape(batch, block_len, kv_here, group_size, head_dim)
    all_keys = jnp.concatenate([key_old, key_new], axis=1)
    all_values = jnp.concatenate([value_old, value_new], axis=1)
    scores = jnp.einsum(
        "btkgd,bskd->bkgts", grouped, all_keys, preferred_element_type=jnp.float32
    ) / math.sqrt(head_dim)
    key_pos = jnp.arange(old_len + block_len, dtype=jnp.int32)
    query_pos = jnp.arange(block_len, dtype=jnp.int32)
    in_prefix = key_pos[None, None, :] < prefix_mine[:, None, None]
    shifted = key_pos - old_len
    in_suffix = (shifted[None, None, :] <= query_pos[None, :, None]) & (
        shifted[None, None, :] < suffix_mine[:, None, None]
    )
    allowed = jnp.where(key_pos[None, None, :] < old_len, in_prefix, in_suffix)[:, None, None]
    masked = jnp.where(allowed, scores, -1e30)
    peak = jnp.max(masked, axis=-1, keepdims=True)
    weights = jnp.where(allowed, jnp.exp(masked - peak), 0.0)
    probs = (weights / jnp.sum(weights, axis=-1, keepdims=True)).astype(jnp.bfloat16)
    mixed = jnp.einsum("bkgts,bskd->btkgd", probs, all_values, preferred_element_type=jnp.float32)
    live = query_pos[None, :] < suffix_mine[:, None]
    mixed = jnp.where(live[:, :, None, None, None], mixed, 0.0)
    return mixed.reshape(batch * block_len, heads_here * head_dim).astype(jnp.bfloat16)


def swap_parts(value):
    count = lax.axis_size("parts")
    return lax.ppermute(value, "parts", [(i, i ^ 1) for i in range(count)])


def swap_cores(value):
    count = lax.axis_size("tp")
    return lax.ppermute(value, "tp", [(i, i ^ 1) for i in range(count)])


def shift_chips(value, by):
    count = lax.axis_size("tp")
    return lax.ppermute(value, "tp", [(i, (i + by * CORES) % count) for i in range(count)])


def gather_chips(own, cut):
    from_left = shift_chips(own, 1)
    from_right = shift_chips(own, -1)
    own_other = swap_cores(own)
    far_top = shift_chips(from_left[:cut], 1)
    far_low = shift_chips(from_right[cut:], -1)
    left_other = swap_cores(from_left)
    right_other = swap_cores(from_right)
    far = jnp.concatenate([far_top, far_low], axis=0)
    far_other = swap_cores(far)
    return (
        (own, own_other),
        (from_left, left_other),
        (from_right, right_other),
        (far, far_other),
    )


GAIN_ROWS = 16
STEPS = (0, -1, 1, 2)
STRIDE = 4


def shift_groups(value, by):
    count = lax.axis_size("seq")
    return lax.ppermute(value, "seq", [(i, (i + by) % count) for i in range(count)])


def gather_near(shard):
    count = lax.axis_size("seq")
    classes = [list(range(c, count, STRIDE)) for c in range(STRIDE)]
    return lax.all_gather(shard, "seq", axis=0, axis_index_groups=classes, tiled=True)


def trade_near(near):
    mid = near.shape[0] // 2
    return (
        near,
        shift_groups(near, -1),
        shift_groups(near, 1),
        shift_groups(near[:mid], 2),
        shift_groups(near[mid:], -2),
    )


def interleave(pieces, rows, my_group):
    near = pieces[0]
    width = near.shape[1]
    blocks = near.shape[0] // rows
    whole = jnp.zeros((blocks, STRIDE, rows, width), near.dtype)
    places = ((0, 0), (1, 0), (-1, 0), (2, 0), (2, blocks // 2))
    for value, (step, start) in zip(pieces, places):
        at = (my_group + step) % STRIDE
        whole = lax.dynamic_update_slice(
            whole, value.reshape(-1, 1, rows, width), (start, at, 0, 0)
        )
    return whole.reshape(blocks * STRIDE * rows, width)


def body(
    tokens,
    norm_gain,
    w_query,
    w_kv,
    b_query,
    b_kv,
    kv_pool,
    prefix_pages,
    prefix_len,
    suffix_len,
    fresh_owner,
):
    seq_count = lax.axis_size("seq")
    tp_count = lax.axis_size("tp")
    my_group = lax.axis_index("seq")
    my_tp = lax.axis_index("tp")
    parity = lax.axis_index("parts") % 2
    token_rows, feat = tokens.shape
    blocks_here = token_rows // BLOCK
    kv_width = w_kv.shape[2]
    kv_here = kv_width // HEAD_DIM
    query_width = w_query.shape[1]
    half_width = query_width // 2
    heads_here = query_width // HEAD_DIM
    half_heads = heads_here // 2
    pool_pages = kv_pool.shape[0]
    page_slots = prefix_pages.shape[1]
    prefix_entries = blocks_here * page_slots
    suffix_pages = BLOCK // PAGE
    fresh_entries = blocks_here * suffix_pages
    prefix_cap = max(3, prefix_entries // seq_count + 1)
    fresh_cap = max(2, (fresh_entries + seq_count - 1) // seq_count + 1)
    first_row = my_group * blocks_here
    prefix_mine = lax.dynamic_slice_in_dim(prefix_len, first_row, blocks_here)
    suffix_mine = lax.dynamic_slice_in_dim(suffix_len, first_row, blocks_here)
    owners_mine = lax.dynamic_slice_in_dim(
        fresh_owner[:, 0], first_row * suffix_pages, fresh_entries
    )

    w_pair_half = lax.dynamic_index_in_dim(w_kv, parity, 1, keepdims=False)
    w_query_half = lax.dynamic_slice_in_dim(w_query, parity * half_width, half_width, axis=1)
    w_query_all = lax.all_gather(w_query_half, "seq", axis=0, tiled=True)
    b_pair_half = lax.dynamic_index_in_dim(b_kv, parity, 0, keepdims=True)
    b_query_half = lax.dynamic_slice_in_dim(b_query, parity * half_width, half_width)[None]

    other_prefix = swap_parts(prefix_mine)
    other_tokens = swap_parts(tokens)
    gain_rows = jnp.broadcast_to(norm_gain[None], (GAIN_ROWS, feat))
    both = jnp.concatenate([gain_rows, tokens, other_tokens], axis=0)
    w_pair_half, both = lax.optimization_barrier((w_pair_half, both))
    pieces = gather_chips(both, GAIN_ROWS + token_rows)
    w_pair_near = gather_near(w_pair_half)
    w_pair_pieces = trade_near(w_pair_near)

    square = jnp.zeros((2 * token_rows, 1), jnp.float32)
    raw = []
    for pair, step in zip(pieces, STEPS):
        for core in range(CORES):
            rows = pair[core][GAIN_ROWS:]
            gain = pair[core][:1]
            at = ((my_tp + step * CORES) % tp_count) ^ core
            wide = rows.astype(jnp.float32)
            square = square + jnp.sum(wide * wide, axis=-1, keepdims=True)
            raw.append((rows, gain, at))
    scale = lax.rsqrt(square / (feat * tp_count) + 1e-06)
    normed = jnp.zeros((2 * token_rows, feat * tp_count), jnp.bfloat16)
    for rows, gain, at in raw:
        done = (rows.astype(jnp.float32) * scale * gain.astype(jnp.float32)).astype(jnp.bfloat16)
        normed = lax.dynamic_update_slice_in_dim(normed, done, at * feat, axis=1)
    w_pair_pieces, normed = lax.optimization_barrier((w_pair_pieces, normed))
    w_pair_all = interleave(w_pair_pieces, w_kv.shape[0], my_group)

    all_ids = prefix_pages.reshape(seq_count, prefix_entries)
    all_owner = all_ids // pool_pages
    entry_ids = jnp.arange(prefix_entries, dtype=jnp.int32)
    before = (all_owner[:, :, None] == all_owner[:, None, :]) & (
        entry_ids[None, None, :] < entry_ids[None, :, None]
    )
    all_rank = jnp.sum(before.astype(jnp.int32), axis=-1)
    prefix_slots = jnp.arange(prefix_cap, dtype=jnp.int32)
    chosen = (all_owner[:, None, :] == my_group) & (
        all_rank[:, None, :] == prefix_slots[None, :, None]
    )
    picked = jnp.sum(jnp.where(chosen, entry_ids[None, None, :], 0), axis=-1)
    local_page = jnp.take_along_axis(all_ids, picked, axis=1) % pool_pages
    prefix_send = kv_pool[local_page]
    prefix_send, _ = lax.optimization_barrier((prefix_send, w_pair_near))
    prefix_got = lax.all_to_all(prefix_send, "seq", split_axis=0, concat_axis=0, tiled=True)

    slot_ids = jnp.arange(BLOCK, dtype=jnp.int32)
    both_prefix = jnp.concatenate([prefix_mine, other_prefix])
    positions = both_prefix[:, None] + slot_ids[None, :]
    live = (slot_ids[None, :] < suffix_mine[:, None])[:, :, None, None]
    pair_lin = jnp.dot(normed, w_pair_all, preferred_element_type=jnp.float32) + b_pair_half
    pair_lin = pair_lin.reshape(2 * blocks_here, BLOCK, kv_here, HEAD_DIM)
    pair_half = jnp.where(parity == 0, rotate(pair_lin, positions), pair_lin).astype(jnp.bfloat16)
    pair_kept = pair_half[:blocks_here]
    pair_got = swap_parts(pair_half[blocks_here:])
    zero = jnp.zeros((), jnp.bfloat16)
    key_new = jnp.where(live, jnp.where(parity == 0, pair_kept, pair_got), zero)
    value_new = jnp.where(live, jnp.where(parity == 0, pair_got, pair_kept), zero)

    new_pages = jnp.stack(
        [
            key_new.reshape(fresh_entries, PAGE, kv_width),
            value_new.reshape(fresh_entries, PAGE, kv_width),
        ],
        axis=1,
    )
    fresh_ids = jnp.arange(fresh_entries, dtype=jnp.int32)
    fresh_before = (owners_mine[None, :] == owners_mine[:, None]) & (
        fresh_ids[None, :] < fresh_ids[:, None]
    )
    fresh_rank = jnp.sum(fresh_before.astype(jnp.int32), axis=1)
    group_ids = jnp.arange(seq_count, dtype=jnp.int32)
    fresh_slots = jnp.arange(fresh_cap, dtype=jnp.int32)
    placed = (owners_mine[None, None, :] == group_ids[:, None, None]) & (
        fresh_rank[None, None, :] == fresh_slots[None, :, None]
    )
    source = jnp.sum(jnp.where(placed, fresh_ids[None, None, :], 0), axis=-1)
    filled = jnp.any(placed, axis=-1)
    fresh_send = jnp.where(filled[:, :, None, None, None], new_pages[source], zero)
    fresh_got = lax.all_to_all(fresh_send, "seq", split_axis=0, concat_axis=0, tiled=True)

    query_lin = jnp.dot(normed, w_query_all, preferred_element_type=jnp.float32) + b_query_half
    query_half = rotate(
        query_lin.reshape(2 * blocks_here, BLOCK, half_heads, HEAD_DIM), positions
    ).astype(jnp.bfloat16)
    query_kept = query_half[:blocks_here]
    query_got = swap_parts(query_half[blocks_here:])
    query = jnp.concatenate(
        [
            jnp.where(parity == 0, query_kept, query_got),
            jnp.where(parity == 0, query_got, query_kept),
        ],
        axis=2,
    )

    my_rank = lax.dynamic_index_in_dim(all_rank, my_group, 0, keepdims=False)
    my_ids = lax.dynamic_index_in_dim(all_ids, my_group, 0, keepdims=False)
    arrived_at = my_ids // pool_pages * prefix_cap + my_rank
    fetched = prefix_got.reshape(seq_count * prefix_cap, 2, PAGE, kv_width)[arrived_at]
    fetched = fetched.reshape(blocks_here, page_slots, 2, PAGE, kv_here, HEAD_DIM)
    key_old = fetched[:, :, 0].reshape(blocks_here, page_slots * PAGE, kv_here, HEAD_DIM)
    value_old = fetched[:, :, 1].reshape(blocks_here, page_slots * PAGE, kv_here, HEAD_DIM)
    attn_out = attend(query, key_new, value_new, key_old, value_old, prefix_mine, suffix_mine)
    fresh_out = fresh_got.reshape(seq_count * fresh_cap, 2, PAGE, kv_width)
    return (attn_out, fresh_out)


def solution(mesh):
    placed = (
        P(("parts", "seq"), "tp"),
        P("tp"),
        P("seq", "tp"),
        P("seq", None, "tp"),
        P("tp"),
        P(None, "tp"),
        P(("parts", "seq"), None, None, "tp"),
        P("parts", None),
        P("parts"),
        P("parts"),
        P("parts", None),
    )
    return jax.shard_map(
        body,
        mesh=mesh,
        in_specs=placed,
        out_specs=(P(("parts", "seq"), "tp"), P(("parts", "seq"), None, None, "tp")),
        check_vma=False,
    )
```

```python
import functools
import math

import jax
import jax.numpy as jnp
from jax import lax
from jax.experimental import pallas as pl
from jax.experimental.pallas import tpu as pltpu
from jax.sharding import PartitionSpec as P


HEAD_DIM = 128
BLOCK = 128
PAGE = 8
CORES = 2


def turn_tables(positions, width):
    half_dim = width // 2
    freq_index = jnp.arange(half_dim, dtype=jnp.float32)
    inverse = jnp.exp(freq_index * (-2.0 * math.log(1000000.0) / width))
    angles = positions.astype(jnp.float32)[:, None] * inverse
    cosine = jnp.cos(angles)
    sine = jnp.sin(angles)
    return cosine, sine


def attend(query, key_new, value_new, key_old, value_old, prefix_mine, suffix_mine):
    batch, block_len, heads_here, head_dim = query.shape
    kv_here = key_new.shape[2]
    group_size = heads_here // kv_here
    old_len = key_old.shape[1]
    grouped = query.reshape(batch, block_len, kv_here, group_size, head_dim)
    all_keys = jnp.concatenate([key_old, key_new], axis=1)
    all_values = jnp.concatenate([value_old, value_new], axis=1)
    scores = jnp.einsum(
        "btkgd,bskd->bkgts", grouped, all_keys, preferred_element_type=jnp.float32
    ) / math.sqrt(head_dim)
    key_pos = jnp.arange(old_len + block_len, dtype=jnp.int32)
    query_pos = jnp.arange(block_len, dtype=jnp.int32)
    in_prefix = key_pos[None, None, :] < prefix_mine[:, None, None]
    shifted = key_pos - old_len
    in_suffix = (shifted[None, None, :] <= query_pos[None, :, None]) & (
        shifted[None, None, :] < suffix_mine[:, None, None]
    )
    allowed = jnp.where(key_pos[None, None, :] < old_len, in_prefix, in_suffix)[:, None, None]
    masked = jnp.where(allowed, scores, -1e30)
    peak = jnp.max(masked, axis=-1, keepdims=True)
    weights = jnp.where(allowed, jnp.exp(masked - peak), 0.0)
    probs = (weights / jnp.sum(weights, axis=-1, keepdims=True)).astype(jnp.bfloat16)
    mixed = jnp.einsum("bkgts,bskd->btkgd", probs, all_values, preferred_element_type=jnp.float32)
    live = query_pos[None, :] < suffix_mine[:, None]
    mixed = jnp.where(live[:, :, None, None, None], mixed, 0.0)
    return mixed.reshape(batch * block_len, heads_here * head_dim).astype(jnp.bfloat16)


def swap_parts(value):
    count = lax.axis_size("parts")
    return lax.ppermute(value, "parts", [(i, i ^ 1) for i in range(count)])


def swap_cores(value):
    count = lax.axis_size("tp")
    return lax.ppermute(value, "tp", [(i, i ^ 1) for i in range(count)])


def shift_chips(value, by):
    count = lax.axis_size("tp")
    return lax.ppermute(value, "tp", [(i, (i + by * CORES) % count) for i in range(count)])


def gather_chips(own, cut):
    from_left = shift_chips(own, 1)
    from_right = shift_chips(own, -1)
    own_other = swap_cores(own)
    far_top = shift_chips(from_left[:cut], 1)
    far_low = shift_chips(from_right[cut:], -1)
    left_other = swap_cores(from_left)
    right_other = swap_cores(from_right)
    far = jnp.concatenate([far_top, far_low], axis=0)
    far_other = swap_cores(far)
    return (
        (own, own_other),
        (from_left, left_other),
        (from_right, right_other),
        (far, far_other),
    )


GAIN_ROWS = 16
STEPS = (0, -1, 1, 2)
STRIDE = 4


def shift_groups(value, by):
    count = lax.axis_size("seq")
    return lax.ppermute(value, "seq", [(i, (i + by) % count) for i in range(count)])


def gather_near(shard):
    count = lax.axis_size("seq")
    classes = [list(range(c, count, STRIDE)) for c in range(STRIDE)]
    return lax.all_gather(shard, "seq", axis=0, axis_index_groups=classes, tiled=True)


def trade_near(near):
    mid = near.shape[0] // 2
    return (
        near,
        shift_groups(near, -1),
        shift_groups(near, 1),
        shift_groups(near[:mid], 2),
        shift_groups(near[mid:], -2),
    )


CHUNK = 32


def pair_kernel(at_ref, *refs, count, shard):
    pieces = refs[:count]
    gains = refs[count : 2 * count]
    weights = refs[2 * count : 2 * count + 5]
    bias_ref, cos_ref, sin_ref, normed_ref, out_ref = refs[2 * count + 5 :]
    rows, feat = pieces[0].shape
    total = feat * len(pieces)

    def chunk(step, carry):
        row = pl.multiple_of(step * CHUNK, CHUNK)
        square = jnp.zeros((CHUNK, 1), jnp.float32)
        for piece in pieces:
            wide = piece[pl.ds(row, CHUNK), :].astype(jnp.float32)
            square = square + jnp.sum(wide * wide, axis=-1, keepdims=True)
        scale = lax.rsqrt(square / total + 1e-06)
        for k, piece in enumerate(pieces):
            wide = piece[pl.ds(row, CHUNK), :].astype(jnp.float32)
            gain = gains[k][:1, :].astype(jnp.float32)
            column = pl.multiple_of(at_ref[k] * feat, feat)
            normed_ref[pl.ds(row, CHUNK), pl.ds(column, feat)] = (wide * scale * gain).astype(
                jnp.bfloat16
            )
        return carry

    lax.fori_loop(0, rows // CHUNK, chunk, 0)
    half = weights[0].shape[0] // shard // 2
    acc = jnp.zeros(out_ref.shape, jnp.float32)
    for k, (weight, start) in enumerate(zip(weights, (0, 0, 0, 0, half))):
        for m in range(weight.shape[0] // shard):
            column = (at_ref[count + k] + STRIDE * (start + m)) * shard
            left = normed_ref[:, pl.ds(pl.multiple_of(column, shard), shard)]
            acc = acc + jnp.dot(
                left, weight[m * shard : (m + 1) * shard, :], preferred_element_type=jnp.float32
            )
    lin = acc + bias_ref[...]
    cosine = jnp.concatenate([cos_ref[...], cos_ref[...]], axis=1)
    sine = jnp.concatenate([-sin_ref[...], sin_ref[...]], axis=1)
    turned = lin * cosine + pltpu.roll(lin, lin.shape[1] // 2, 1) * sine
    out_ref[...] = turned.astype(jnp.bfloat16)


def project_pair(at, pieces, weights, shard, bias, cosine, sine):
    height, feat = pieces[0].shape
    tokens = height - GAIN_ROWS
    rows = tokens // 4
    width = weights[0].shape[1]
    whole = lambda a: pl.BlockSpec(a.shape, lambda i: (0, 0))
    by_rows = lambda w: pl.BlockSpec((rows, w), lambda i: (i, 0))
    gain_at = tokens // GAIN_ROWS
    return pl.pallas_call(
        functools.partial(pair_kernel, count=len(pieces), shard=shard),
        grid=(4,),
        in_specs=[pl.BlockSpec(memory_space=pltpu.SMEM)]
        + [by_rows(feat) for _ in pieces]
        + [pl.BlockSpec((GAIN_ROWS, feat), lambda i: (gain_at, 0)) for _ in pieces]
        + [whole(w) for w in weights]
        + [whole(bias), by_rows(width // 2), by_rows(width // 2)],
        out_specs=[by_rows(feat * len(pieces)), by_rows(width)],
        out_shape=[
            jax.ShapeDtypeStruct((tokens, feat * len(pieces)), jnp.bfloat16),
            jax.ShapeDtypeStruct((tokens, width), jnp.bfloat16),
        ],
    )(at, *pieces, *pieces, *weights, bias, cosine, sine)


def body(
    tokens,
    norm_gain,
    w_query,
    w_kv,
    b_query,
    b_kv,
    kv_pool,
    prefix_pages,
    prefix_len,
    suffix_len,
    fresh_owner,
):
    seq_count = lax.axis_size("seq")
    tp_count = lax.axis_size("tp")
    my_group = lax.axis_index("seq")
    my_tp = lax.axis_index("tp")
    parity = lax.axis_index("parts") % 2
    token_rows, feat = tokens.shape
    blocks_here = token_rows // BLOCK
    kv_width = w_kv.shape[2]
    kv_here = kv_width // HEAD_DIM
    query_width = w_query.shape[1]
    half_width = query_width // 2
    heads_here = query_width // HEAD_DIM
    half_heads = heads_here // 2
    pool_pages = kv_pool.shape[0]
    page_slots = prefix_pages.shape[1]
    prefix_entries = blocks_here * page_slots
    suffix_pages = BLOCK // PAGE
    fresh_entries = blocks_here * suffix_pages
    prefix_cap = max(3, prefix_entries // seq_count + 1)
    fresh_cap = max(2, (fresh_entries + seq_count - 1) // seq_count + 1)
    first_row = my_group * blocks_here
    prefix_mine = lax.dynamic_slice_in_dim(prefix_len, first_row, blocks_here)
    suffix_mine = lax.dynamic_slice_in_dim(suffix_len, first_row, blocks_here)
    w_query_half = lax.dynamic_slice_in_dim(w_query, parity * half_width, half_width, axis=1)
    w_query_half, w_kv = lax.optimization_barrier((w_query_half, w_kv))
    w_query_all = lax.all_gather(w_query_half, "seq", axis=0, tiled=True)
    w_pair_half = lax.dynamic_index_in_dim(w_kv, parity, 1, keepdims=False)
    w_pair_half, tokens, prefix_mine = lax.optimization_barrier((w_pair_half, tokens, prefix_mine))
    b_pair_half = lax.dynamic_index_in_dim(b_kv, parity, 0, keepdims=True)
    b_query_half = lax.dynamic_slice_in_dim(b_query, parity * half_width, half_width)[None]

    other_tokens = swap_parts(tokens)
    other_prefix = swap_parts(prefix_mine)
    w_pair_near = gather_near(w_pair_half)
    prefix_pages, fresh_owner, w_pair_near, other_tokens = lax.optimization_barrier(
        (prefix_pages, fresh_owner, w_pair_near, other_tokens)
    )
    owners_mine = lax.dynamic_slice_in_dim(
        fresh_owner[:, 0], first_row * suffix_pages, fresh_entries
    )
    w_pair_pieces = trade_near(w_pair_near)
    gain_rows = jnp.broadcast_to(norm_gain[None], (GAIN_ROWS, feat))
    both = jnp.concatenate([tokens, other_tokens, gain_rows], axis=0)
    pieces = gather_chips(both, token_rows)
    flat = [pair[core] for pair in pieces for core in range(CORES)]
    turns = jnp.array([step * CORES for step in STEPS for _ in range(CORES)], jnp.int32)
    cores = jnp.array([core for _ in STEPS for core in range(CORES)], jnp.int32)
    near_steps = jnp.array([0, 1, -1, 2, 2], jnp.int32)
    at = jnp.concatenate(
        [((my_tp + turns) % tp_count) ^ cores, (my_group + near_steps) % STRIDE]
    )

    all_ids = prefix_pages.reshape(seq_count, prefix_entries)
    all_owner = all_ids // pool_pages
    entry_ids = jnp.arange(prefix_entries, dtype=jnp.int32)
    before = (all_owner[:, :, None] == all_owner[:, None, :]) & (
        entry_ids[None, None, :] < entry_ids[None, :, None]
    )
    all_rank = jnp.sum(before.astype(jnp.int32), axis=-1)
    prefix_slots = jnp.arange(prefix_cap, dtype=jnp.int32)
    chosen = (all_owner[:, None, :] == my_group) & (
        all_rank[:, None, :] == prefix_slots[None, :, None]
    )
    picked = jnp.sum(jnp.where(chosen, entry_ids[None, None, :], 0), axis=-1)
    local_page = jnp.take_along_axis(all_ids, picked, axis=1) % pool_pages
    prefix_send = kv_pool[local_page]
    prefix_got = lax.all_to_all(prefix_send, "seq", split_axis=0, concat_axis=0, tiled=True)

    slot_ids = jnp.arange(BLOCK, dtype=jnp.int32)
    both_prefix = jnp.concatenate([prefix_mine, other_prefix])
    positions = (both_prefix[:, None] + slot_ids[None, :]).reshape(-1)
    live = (slot_ids[None, :] < suffix_mine[:, None])[:, :, None, None]
    cosine, sine = turn_tables(positions, HEAD_DIM)
    pair_cosine = jnp.where(parity == 0, cosine, 1.0)
    pair_sine = jnp.where(parity == 0, sine, 0.0)
    normed, pair_half = project_pair(
        at, flat, w_pair_pieces, w_kv.shape[0], b_pair_half.reshape(1, kv_width), pair_cosine, pair_sine
    )
    pair_half = pair_half.reshape(2 * blocks_here, BLOCK, kv_here, HEAD_DIM)
    pair_kept = pair_half[:blocks_here]
    pair_got = swap_parts(pair_half[blocks_here:])
    zero = jnp.zeros((), jnp.bfloat16)
    key_new = jnp.where(live, jnp.where(parity == 0, pair_kept, pair_got), zero)
    value_new = jnp.where(live, jnp.where(parity == 0, pair_got, pair_kept), zero)

    new_pages = jnp.stack(
        [
            key_new.reshape(fresh_entries, PAGE, kv_width),
            value_new.reshape(fresh_entries, PAGE, kv_width),
        ],
        axis=1,
    )
    fresh_ids = jnp.arange(fresh_entries, dtype=jnp.int32)
    fresh_before = (owners_mine[None, :] == owners_mine[:, None]) & (
        fresh_ids[None, :] < fresh_ids[:, None]
    )
    fresh_rank = jnp.sum(fresh_before.astype(jnp.int32), axis=1)
    group_ids = jnp.arange(seq_count, dtype=jnp.int32)
    fresh_slots = jnp.arange(fresh_cap, dtype=jnp.int32)
    placed = (owners_mine[None, None, :] == group_ids[:, None, None]) & (
        fresh_rank[None, None, :] == fresh_slots[None, :, None]
    )
    source = jnp.sum(jnp.where(placed, fresh_ids[None, None, :], 0), axis=-1)
    filled = jnp.any(placed, axis=-1)
    fresh_send = jnp.where(filled[:, :, None, None, None], new_pages[source], zero)
    fresh_got = lax.all_to_all(fresh_send, "seq", split_axis=0, concat_axis=0, tiled=True)

    query_lin = jnp.dot(normed, w_query_all, preferred_element_type=jnp.float32) + b_query_half
    query_lin = query_lin.reshape(2 * blocks_here * BLOCK, half_heads, HEAD_DIM)
    first, second = jnp.split(query_lin, 2, axis=-1)
    query_half = jnp.concatenate(
        [
            first * cosine[:, None, :] - second * sine[:, None, :],
            second * cosine[:, None, :] + first * sine[:, None, :],
        ],
        axis=-1,
    )
    query_half = query_half.astype(jnp.bfloat16)
    query_half = query_half.reshape(2 * blocks_here, BLOCK, half_heads, HEAD_DIM)
    query_kept = query_half[:blocks_here]
    query_got = swap_parts(query_half[blocks_here:])
    query = jnp.concatenate(
        [
            jnp.where(parity == 0, query_kept, query_got),
            jnp.where(parity == 0, query_got, query_kept),
        ],
        axis=2,
    )

    my_rank = lax.dynamic_index_in_dim(all_rank, my_group, 0, keepdims=False)
    my_ids = lax.dynamic_index_in_dim(all_ids, my_group, 0, keepdims=False)
    arrived_at = my_ids // pool_pages * prefix_cap + my_rank
    fetched = prefix_got.reshape(seq_count * prefix_cap, 2, PAGE, kv_width)[arrived_at]
    fetched = fetched.reshape(blocks_here, page_slots, 2, PAGE, kv_here, HEAD_DIM)
    key_old = fetched[:, :, 0].reshape(blocks_here, page_slots * PAGE, kv_here, HEAD_DIM)
    value_old = fetched[:, :, 1].reshape(blocks_here, page_slots * PAGE, kv_here, HEAD_DIM)
    attn_out = attend(query, key_new, value_new, key_old, value_old, prefix_mine, suffix_mine)
    fresh_out = fresh_got.reshape(seq_count * fresh_cap, 2, PAGE, kv_width)
    return (attn_out, fresh_out)


def solution(mesh):
    placed = (
        P(("parts", "seq"), "tp"),
        P("tp"),
        P("seq", "tp"),
        P("seq", None, "tp"),
        P("tp"),
        P(None, "tp"),
        P(("parts", "seq"), None, None, "tp"),
        P("parts", None),
        P("parts"),
        P("parts"),
        P("parts", None),
    )

    return jax.shard_map(
        body,
        mesh=mesh,
        in_specs=placed,
        out_specs=(P(("parts", "seq"), "tp"), P(("parts", "seq"), None, None, "tp")),
        check_vma=False,
    )
```

```python
import functools
import math

import jax
import jax.numpy as jnp
from jax import lax
from jax.experimental import pallas as pl
from jax.experimental.pallas import tpu as pltpu
from jax.sharding import PartitionSpec as P


HEAD_DIM = 128
BLOCK = 128
PAGE = 8
CORES = 2


def turn_tables(positions, width):
    half_dim = width // 2
    freq_index = jnp.arange(half_dim, dtype=jnp.float32)
    inverse = jnp.exp(freq_index * (-2.0 * math.log(1000000.0) / width))
    angles = positions.astype(jnp.float32)[:, None] * inverse
    cosine = jnp.cos(angles)
    sine = jnp.sin(angles)
    return cosine, sine


def attend(query, key_new, value_new, key_old, value_old, prefix_mine, suffix_mine):
    batch, block_len, heads_here, head_dim = query.shape
    kv_here = key_new.shape[2]
    group_size = heads_here // kv_here
    old_len = key_old.shape[1]
    grouped = query.reshape(batch, block_len, kv_here, group_size, head_dim)
    all_keys = jnp.concatenate([key_old, key_new], axis=1)
    all_values = jnp.concatenate([value_old, value_new], axis=1)
    scores = jnp.einsum(
        "btkgd,bskd->bkgts", grouped, all_keys, preferred_element_type=jnp.float32
    ) / math.sqrt(head_dim)
    key_pos = jnp.arange(old_len + block_len, dtype=jnp.int32)
    query_pos = jnp.arange(block_len, dtype=jnp.int32)
    in_prefix = key_pos[None, None, :] < prefix_mine[:, None, None]
    shifted = key_pos - old_len
    in_suffix = (shifted[None, None, :] <= query_pos[None, :, None]) & (
        shifted[None, None, :] < suffix_mine[:, None, None]
    )
    allowed = jnp.where(key_pos[None, None, :] < old_len, in_prefix, in_suffix)[:, None, None]
    masked = jnp.where(allowed, scores, -1e30)
    peak = jnp.max(masked, axis=-1, keepdims=True)
    weights = jnp.where(allowed, jnp.exp(masked - peak), 0.0)
    probs = (weights / jnp.sum(weights, axis=-1, keepdims=True)).astype(jnp.bfloat16)
    mixed = jnp.einsum("bkgts,bskd->btkgd", probs, all_values, preferred_element_type=jnp.float32)
    live = query_pos[None, :] < suffix_mine[:, None]
    mixed = jnp.where(live[:, :, None, None, None], mixed, 0.0)
    return mixed.reshape(batch * block_len, heads_here * head_dim).astype(jnp.bfloat16)


def swap_parts(value):
    count = lax.axis_size("parts")
    return lax.ppermute(value, "parts", [(i, i ^ 1) for i in range(count)])


def swap_cores(value):
    count = lax.axis_size("tp")
    return lax.ppermute(value, "tp", [(i, i ^ 1) for i in range(count)])


def shift_chips(value, by):
    count = lax.axis_size("tp")
    return lax.ppermute(value, "tp", [(i, (i + by * CORES) % count) for i in range(count)])


def gather_chips(own, cut):
    from_left = shift_chips(own, 1)
    from_right = shift_chips(own, -1)
    own_other = swap_cores(own)
    far_top = shift_chips(from_left[:cut], 1)
    far_low = shift_chips(from_right[cut:], -1)
    left_other = swap_cores(from_left)
    right_other = swap_cores(from_right)
    far = jnp.concatenate([far_top, far_low], axis=0)
    far_other = swap_cores(far)
    return (
        (own, own_other),
        (from_left, left_other),
        (from_right, right_other),
        (far, far_other),
    )


GAIN_ROWS = 16
STEPS = (0, -1, 1, 2)
STRIDE = 4


def shift_groups(value, by):
    count = lax.axis_size("seq")
    return lax.ppermute(value, "seq", [(i, (i + by) % count) for i in range(count)])


def gather_near(shard):
    count = lax.axis_size("seq")
    classes = [list(range(c, count, STRIDE)) for c in range(STRIDE)]
    return lax.all_gather(shard, "seq", axis=0, axis_index_groups=classes, tiled=True)


def trade_near(near):
    mid = near.shape[0] // 2
    return (
        near,
        shift_groups(near, -1),
        shift_groups(near, 1),
        shift_groups(near[:mid], 2),
        shift_groups(near[mid:], -2),
    )


CHUNK = 32


def pair_kernel(at_ref, *refs, count, shard):
    pieces = refs[:count]
    gains = refs[count : 2 * count]
    weights = refs[2 * count : 2 * count + 5]
    bias_ref, cos_ref, sin_ref, normed_ref, out_ref = refs[2 * count + 5 :]
    rows, feat = pieces[0].shape
    total = feat * len(pieces)

    def chunk(step, carry):
        row = pl.multiple_of(step * CHUNK, CHUNK)
        square = jnp.zeros((CHUNK, 1), jnp.float32)
        for piece in pieces:
            wide = piece[pl.ds(row, CHUNK), :].astype(jnp.float32)
            square = square + jnp.sum(wide * wide, axis=-1, keepdims=True)
        scale = lax.rsqrt(square / total + 1e-06)
        for k, piece in enumerate(pieces):
            wide = piece[pl.ds(row, CHUNK), :].astype(jnp.float32)
            gain = gains[k][:1, :].astype(jnp.float32)
            column = pl.multiple_of(at_ref[k] * feat, feat)
            normed_ref[pl.ds(row, CHUNK), pl.ds(column, feat)] = (wide * scale * gain).astype(
                jnp.bfloat16
            )
        return carry

    lax.fori_loop(0, rows // CHUNK, chunk, 0)
    half = weights[0].shape[0] // shard // 2
    acc = jnp.zeros(out_ref.shape, jnp.float32)
    for k, (weight, start) in enumerate(zip(weights, (0, 0, 0, 0, half))):
        for m in range(weight.shape[0] // shard):
            column = (at_ref[count + k] + STRIDE * (start + m)) * shard
            left = normed_ref[:, pl.ds(pl.multiple_of(column, shard), shard)]
            acc = acc + jnp.dot(
                left, weight[m * shard : (m + 1) * shard, :], preferred_element_type=jnp.float32
            )
    lin = acc + bias_ref[...]
    cosine = jnp.concatenate([cos_ref[...], cos_ref[...]], axis=1)
    sine = jnp.concatenate([-sin_ref[...], sin_ref[...]], axis=1)
    turned = lin * cosine + pltpu.roll(lin, lin.shape[1] // 2, 1) * sine
    out_ref[...] = turned.astype(jnp.bfloat16)


def project_pair(at, pieces, weights, shard, bias, cosine, sine):
    height, feat = pieces[0].shape
    tokens = height - GAIN_ROWS
    rows = tokens // 4
    width = weights[0].shape[1]
    whole = lambda a: pl.BlockSpec(a.shape, lambda i: (0, 0))
    by_rows = lambda w: pl.BlockSpec((rows, w), lambda i: (i, 0))
    gain_at = tokens // GAIN_ROWS
    return pl.pallas_call(
        functools.partial(pair_kernel, count=len(pieces), shard=shard),
        grid=(4,),
        in_specs=[pl.BlockSpec(memory_space=pltpu.SMEM)]
        + [by_rows(feat) for _ in pieces]
        + [pl.BlockSpec((GAIN_ROWS, feat), lambda i: (gain_at, 0)) for _ in pieces]
        + [whole(w) for w in weights]
        + [whole(bias), by_rows(width // 2), by_rows(width // 2)],
        out_specs=[by_rows(feat * len(pieces)), by_rows(width)],
        out_shape=[
            jax.ShapeDtypeStruct((tokens, feat * len(pieces)), jnp.bfloat16),
            jax.ShapeDtypeStruct((tokens, width), jnp.bfloat16),
        ],
    )(at, *pieces, *pieces, *weights, bias, cosine, sine)


def body(
    tokens,
    norm_gain,
    w_query,
    w_kv,
    b_query,
    b_kv,
    kv_pool,
    prefix_pages,
    prefix_len,
    suffix_len,
    fresh_owner,
):
    seq_count = lax.axis_size("seq")
    tp_count = lax.axis_size("tp")
    my_group = lax.axis_index("seq")
    my_tp = lax.axis_index("tp")
    parity = lax.axis_index("parts") % 2
    token_rows, feat = tokens.shape
    blocks_here = token_rows // BLOCK
    kv_width = w_kv.shape[2]
    kv_here = kv_width // HEAD_DIM
    query_width = w_query.shape[1]
    half_width = query_width // 2
    heads_here = query_width // HEAD_DIM
    half_heads = heads_here // 2
    pool_pages = kv_pool.shape[0]
    page_slots = prefix_pages.shape[1]
    prefix_entries = blocks_here * page_slots
    suffix_pages = BLOCK // PAGE
    fresh_entries = blocks_here * suffix_pages
    prefix_cap = max(3, prefix_entries // seq_count + 1)
    fresh_cap = max(2, (fresh_entries + seq_count - 1) // seq_count + 1)
    first_row = my_group * blocks_here
    prefix_mine = lax.dynamic_slice_in_dim(prefix_len, first_row, blocks_here)
    suffix_mine = lax.dynamic_slice_in_dim(suffix_len, first_row, blocks_here)
    w_query_half = lax.dynamic_slice_in_dim(w_query, parity * half_width, half_width, axis=1)
    w_query_half, w_kv = lax.optimization_barrier((w_query_half, w_kv))
    w_query_all = lax.all_gather(w_query_half, "seq", axis=0, tiled=True)
    w_pair_half = lax.dynamic_index_in_dim(w_kv, parity, 1, keepdims=False)
    w_pair_half, tokens, prefix_mine = lax.optimization_barrier((w_pair_half, tokens, prefix_mine))
    b_pair_half = lax.dynamic_index_in_dim(b_kv, parity, 0, keepdims=True)
    b_query_half = lax.dynamic_slice_in_dim(b_query, parity * half_width, half_width)[None]

    other_tokens = swap_parts(tokens)
    other_prefix = swap_parts(prefix_mine)
    w_pair_near = gather_near(w_pair_half)
    prefix_pages, w_pair_near, other_tokens = lax.optimization_barrier(
        (prefix_pages, w_pair_near, other_tokens)
    )
    w_pair_pieces = trade_near(w_pair_near)
    gain_rows = jnp.broadcast_to(norm_gain[None], (GAIN_ROWS, feat))
    both = jnp.concatenate([tokens, other_tokens, gain_rows], axis=0)
    pieces = gather_chips(both, token_rows)
    flat = [pair[core] for pair in pieces for core in range(CORES)]
    turns = jnp.array([step * CORES for step in STEPS for _ in range(CORES)], jnp.int32)
    cores = jnp.array([core for _ in STEPS for core in range(CORES)], jnp.int32)
    near_steps = jnp.array([0, 1, -1, 2, 2], jnp.int32)
    at = jnp.concatenate(
        [((my_tp + turns) % tp_count) ^ cores, (my_group + near_steps) % STRIDE]
    )

    all_ids = prefix_pages.reshape(seq_count, prefix_entries)
    all_owner = all_ids // pool_pages
    entry_ids = jnp.arange(prefix_entries, dtype=jnp.int32)
    before = (all_owner[:, :, None] == all_owner[:, None, :]) & (
        entry_ids[None, None, :] < entry_ids[None, :, None]
    )
    all_rank = jnp.sum(before.astype(jnp.int32), axis=-1)
    prefix_slots = jnp.arange(prefix_cap, dtype=jnp.int32)
    chosen = (all_owner[:, None, :] == my_group) & (
        all_rank[:, None, :] == prefix_slots[None, :, None]
    )
    picked = jnp.sum(jnp.where(chosen, entry_ids[None, None, :], 0), axis=-1)
    local_page = jnp.take_along_axis(all_ids, picked, axis=1) % pool_pages
    prefix_send = kv_pool[local_page]
    fresh_owner, prefix_send = lax.optimization_barrier((fresh_owner, prefix_send))
    owners_mine = lax.dynamic_slice_in_dim(
        fresh_owner[:, 0], first_row * suffix_pages, fresh_entries
    )
    prefix_got = lax.all_to_all(prefix_send, "seq", split_axis=0, concat_axis=0, tiled=True)

    slot_ids = jnp.arange(BLOCK, dtype=jnp.int32)
    both_prefix = jnp.concatenate([prefix_mine, other_prefix])
    positions = (both_prefix[:, None] + slot_ids[None, :]).reshape(-1)
    live = (slot_ids[None, :] < suffix_mine[:, None])[:, :, None, None]
    cosine, sine = turn_tables(positions, HEAD_DIM)
    pair_cosine = jnp.where(parity == 0, cosine, 1.0)
    pair_sine = jnp.where(parity == 0, sine, 0.0)
    normed, pair_half = project_pair(
        at, flat, w_pair_pieces, w_kv.shape[0], b_pair_half.reshape(1, kv_width), pair_cosine, pair_sine
    )
    pair_half = pair_half.reshape(2 * blocks_here, BLOCK, kv_here, HEAD_DIM)
    pair_kept = pair_half[:blocks_here]
    pair_got = swap_parts(pair_half[blocks_here:])
    zero = jnp.zeros((), jnp.bfloat16)
    key_new = jnp.where(live, jnp.where(parity == 0, pair_kept, pair_got), zero)
    value_new = jnp.where(live, jnp.where(parity == 0, pair_got, pair_kept), zero)

    new_pages = jnp.stack(
        [
            key_new.reshape(fresh_entries, PAGE, kv_width),
            value_new.reshape(fresh_entries, PAGE, kv_width),
        ],
        axis=1,
    )
    fresh_ids = jnp.arange(fresh_entries, dtype=jnp.int32)
    fresh_before = (owners_mine[None, :] == owners_mine[:, None]) & (
        fresh_ids[None, :] < fresh_ids[:, None]
    )
    fresh_rank = jnp.sum(fresh_before.astype(jnp.int32), axis=1)
    group_ids = jnp.arange(seq_count, dtype=jnp.int32)
    fresh_slots = jnp.arange(fresh_cap, dtype=jnp.int32)
    placed = (owners_mine[None, None, :] == group_ids[:, None, None]) & (
        fresh_rank[None, None, :] == fresh_slots[None, :, None]
    )
    source = jnp.sum(jnp.where(placed, fresh_ids[None, None, :], 0), axis=-1)
    filled = jnp.any(placed, axis=-1)
    fresh_send = jnp.where(filled[:, :, None, None, None], new_pages[source], zero)
    fresh_got = lax.all_to_all(fresh_send, "seq", split_axis=0, concat_axis=0, tiled=True)

    query_lin = jnp.dot(normed, w_query_all, preferred_element_type=jnp.float32) + b_query_half
    query_lin = query_lin.reshape(2 * blocks_here * BLOCK, half_heads, HEAD_DIM)
    first, second = jnp.split(query_lin, 2, axis=-1)
    query_half = jnp.concatenate(
        [
            first * cosine[:, None, :] - second * sine[:, None, :],
            second * cosine[:, None, :] + first * sine[:, None, :],
        ],
        axis=-1,
    )
    query_half = query_half.astype(jnp.bfloat16)
    query_half = query_half.reshape(2 * blocks_here, BLOCK, half_heads, HEAD_DIM)
    query_kept = query_half[:blocks_here]
    query_got = swap_parts(query_half[blocks_here:])
    query = jnp.concatenate(
        [
            jnp.where(parity == 0, query_kept, query_got),
            jnp.where(parity == 0, query_got, query_kept),
        ],
        axis=2,
    )

    my_rank = lax.dynamic_index_in_dim(all_rank, my_group, 0, keepdims=False)
    my_ids = lax.dynamic_index_in_dim(all_ids, my_group, 0, keepdims=False)
    arrived_at = my_ids // pool_pages * prefix_cap + my_rank
    fetched = prefix_got.reshape(seq_count * prefix_cap, 2, PAGE, kv_width)[arrived_at]
    fetched = fetched.reshape(blocks_here, page_slots, 2, PAGE, kv_here, HEAD_DIM)
    key_old = fetched[:, :, 0].reshape(blocks_here, page_slots * PAGE, kv_here, HEAD_DIM)
    value_old = fetched[:, :, 1].reshape(blocks_here, page_slots * PAGE, kv_here, HEAD_DIM)
    attn_out = attend(query, key_new, value_new, key_old, value_old, prefix_mine, suffix_mine)
    fresh_out = fresh_got.reshape(seq_count * fresh_cap, 2, PAGE, kv_width)
    return (attn_out, fresh_out)


def solution(mesh):
    placed = (
        P(("parts", "seq"), "tp"),
        P("tp"),
        P("seq", "tp"),
        P("seq", None, "tp"),
        P("tp"),
        P(None, "tp"),
        P(("parts", "seq"), None, None, "tp"),
        P("parts", None),
        P("parts"),
        P("parts"),
        P("parts", None),
    )

    return jax.shard_map(
        body,
        mesh=mesh,
        in_specs=placed,
        out_specs=(P(("parts", "seq"), "tp"), P(("parts", "seq"), None, None, "tp")),
        check_vma=False,
    )
```
